256 devices in a mesh: span: 16 (over y, x), model: 16 (over z, core).
Axes of the slice: x: 4, y: 4, z: 8, core: 2. Of those that a mesh axis runs over, the one named last changes fastest.
Arguments:
- latents: bfloat16 [16, 8192, 512], P(None, ('span', 'model')), may hold values from -6 to 6
- rotary_rows: bfloat16 [16, 8192, 64], P(None, ('span', 'model')), may hold values from -6 to 6
- latent_gain: float32 [512], replicated, may hold values from 0.25 to 1.75
- key_up: bfloat16 [512, 16, 128], P(None, 'model'), may hold values from -0.25 to 0.25
- value_up: bfloat16 [512, 16, 128], P(None, 'model'), may hold values from -0.25 to 0.25
Outputs:
- decode_keys: bfloat16 [16, 16, 192, 8192], P('span', 'model')
- decode_values: bfloat16 [16, 8192, 16, 128], P('span', None, 'model')
The draws below stay inside these ranges and needn't reach their ends.
All inputs are finite; a program needn't handle non-finite values.
Results may differ from the reference program's by a relative error of at most 0.0049.
Values may be sent and summed in bfloat16 or wider, within the bound.
A program may use at most 64 MiB of HBM per device.

```python
import jax
import jax.numpy as jnp
from jax import lax

BATCH = 16
LENGTH = 8192
HEADS = 16
LATENT = 512
KEY_PART = 128
ROTARY = 64
VALUE_SIZE = 128


def block_levels(own_key, dims, pieces, smallest, high):
    factor_of, own = 1.0, jax.random.fold_in(own_key, 6)
    for dim, shards_of in pieces:
        heights = jnp.exp(jax.random.uniform(jax.random.fold_in(own, dim), (shards_of,), jnp.float32, smallest / len(pieces), high / len(pieces)))
        factor_of = factor_of * jnp.repeat(heights, dims[dim] // shards_of).reshape([-1 if axis == dim else 1 for axis in range(len(dims))])
    return factor_of


def normal_values(own_key, shape, scale, most, cuts=(), dtype=jnp.bfloat16):
    loudness = block_levels(own_key, shape, cuts, -0.22, 0.18) if cuts else 1.0
    entries = jax.random.normal(own_key, shape, jnp.float32) * scale * loudness
    return jnp.minimum(jnp.maximum(entries, -most), most).astype(dtype)


def setup_inputs(seed: int = 0) -> dict:
    streams_of = jax.random.split(jax.random.key(seed), 6)
    return {
        "latents": normal_values(streams_of[0], (BATCH, LENGTH, LATENT), 1.0, 6.0, ((1, 256),)),
        "rotary_rows": normal_values(streams_of[1], (BATCH, LENGTH, ROTARY), 1.0, 6.0, ((1, 256),)),
        "latent_gain": jnp.clip(1.0 + 0.15 * jax.random.normal(streams_of[2], (LATENT,), jnp.float32), 0.25, 1.75),
        "key_up": normal_values(streams_of[3], (LATENT, HEADS, KEY_PART), LATENT ** -0.5, 0.25, ((1, 16),)),
        "value_up": normal_values(streams_of[4], (LATENT, HEADS, VALUE_SIZE), LATENT ** -0.5, 0.25, ((1, 16),)),
    }


def scale_rows(vectors, row_gain):
    return vectors * lax.rsqrt(lax.optimization_barrier(jnp.mean(vectors * vectors, axis=-1, keepdims=True)) + 1e-06) * row_gain

def reference(latents, rotary_rows, latent_gain, key_up, value_up):
    rows_ready = scale_rows(latents.astype(jnp.float32), latent_gain).astype(jnp.bfloat16)
    rows_ready = lax.optimization_barrier(rows_ready)

    def expand_one(one):
        rows_one, rotary_one = one
        wide_keys = jnp.einsum('tr,rhk->thk', rows_one.astype(jnp.float32), key_up.astype(jnp.float32)).astype(jnp.bfloat16)
        shared = jnp.broadcast_to(rotary_one[:, None], (LENGTH, HEADS, ROTARY))
        wide_values = jnp.einsum('tr,rhk->thk', rows_one.astype(jnp.float32), value_up.astype(jnp.float32)).astype(jnp.bfloat16)
        return (jnp.concatenate([wide_keys, shared], axis=-1), wide_values)
    decode_keys, decode_values = lax.map(expand_one, (rows_ready, rotary_rows))
    decode_keys = jnp.transpose(decode_keys, (0, 2, 3, 1))
    return (decode_keys, decode_values)
```

```python
import functools

import jax
import jax.numpy as jnp
from jax import lax
from jax.experimental import pallas as pl
from jax.experimental.pallas import tpu as pltpu
from jax.sharding import PartitionSpec as P

MESH = pl.DeviceIdType.MESH
LAG = 2
LANES = 128


def tile_of(blocks, gain_ref, wk_ref, wv_ref, groups, wide):
    depth = groups * LANES
    x = [
        jnp.concatenate([b[g * wide : (g + 1) * wide] for b in blocks], axis=0).astype(jnp.float32)
        for g in range(groups)
    ]
    squares = functools.reduce(lambda a, b: a + b, [v * v for v in x])
    scale = lax.rsqrt(jnp.sum(squares, axis=-1, keepdims=True) / depth + 1e-06)
    rows = jnp.concatenate(
        [
            (x[g] * scale * gain_ref[:, g * LANES : (g + 1) * LANES]).astype(jnp.bfloat16)
            for g in range(groups)
        ],
        axis=1,
    )
    values = jnp.dot(rows, wv_ref[...], preferred_element_type=jnp.float32).astype(jnp.bfloat16)
    keys = lax.dot_general(
        wk_ref[...], rows, (((1,), (1,)), ((), ())), preferred_element_type=jnp.float32
    ).astype(jnp.bfloat16)
    turned = []
    for b in blocks:
        packed = b[groups * wide :].astype(jnp.float32)
        turned.append(packed)
        turned.append(pltpu.roll(packed, LANES // 2, 1))
    both = jnp.concatenate(turned, axis=0).astype(jnp.bfloat16)
    eye = (
        lax.broadcasted_iota(jnp.int32, (LANES // 2, LANES), 0)
        == lax.broadcasted_iota(jnp.int32, (LANES // 2, LANES), 1)
    ).astype(jnp.bfloat16)
    rotary = lax.dot_general(
        eye, both, (((1,), (1,)), ((), ())), preferred_element_type=jnp.float32
    ).astype(jnp.bfloat16)
    return keys, rotary, values


def exchange(
    lat_hbm, rot_hbm, gain_hbm, wk_hbm, wv_hbm,
    keys_ref, values_ref,
    pack, rows, rot, gain, wk, wv, wkt,
    in_sems, own_sem, a_send, z_send, c_send, a_recv, p_recv, m_recv, cown_recv, cp_recv, cm_recv,
):
    span, model = lax.axis_index("span"), lax.axis_index("model")
    z, c = model // 2, lax.rem(model, 2)
    up = lax.rem(model + 2, 16)
    down = lax.rem(model + 14, 16)
    other = model + 1 - 2 * c
    wide = lat_hbm.shape[1]
    groups = lat_hbm.shape[2] // LANES

    barrier = pltpu.get_barrier_semaphore()
    for k in range(1, 16):
        pl.semaphore_signal(barrier, inc=1, device_id=(span ^ k, model), device_id_type=MESH)
    for m in (up, down, other):
        pl.semaphore_signal(barrier, inc=1, device_id=(span, m), device_id_type=MESH)

    loads = [
        pltpu.make_async_copy(
            lat_hbm.at[:, :, pl.ds(g * LANES, LANES)],
            pack.at[:, pl.ds(g * wide, wide), :],
            in_sems.at[g],
        )
        for g in range(groups)
    ]
    rot_load = pltpu.make_async_copy(rot_hbm, rot, in_sems.at[groups])
    others = [
        pltpu.make_async_copy(a, b, in_sems.at[groups + 1 + i])
        for i, (a, b) in enumerate(((gain_hbm, gain), (wk_hbm, wk), (wv_hbm, wv)))
    ]
    rot_load.start()
    for d in loads + others:
        d.start()
    rot_load.wait()
    for d in loads:
        d.wait()
    half = wide // 2
    pack[:, groups * wide :, :] = jnp.concatenate([rot[:, :half, :], rot[:, half:, :]], axis=-1)
    for d in others:
        d.wait()
    wkt[...] = wk[...].T

    pl.semaphore_wait(barrier, 18)

    def send(src, dst, send_sem, recv_sem, s, m):
        return pltpu.make_async_remote_copy(
            src_ref=src, dst_ref=dst, send_sem=send_sem, recv_sem=recv_sem,
            device_id=(s, m), device_id_type=MESH,
        )

    own = pltpu.make_async_copy(pack.at[span], rows.at[model, 0], own_sem)

    def hand_on(src, m, k, zs, up_sem, down_sem, core_sem):
        dst = rows.at[m, k]
        if up_sem is not None:
            send(src, dst, z_send.at[zs], up_sem, span, up).start()
        if down_sem is not None:
            send(src, dst, z_send.at[zs], down_sem, span, down).start()
        if core_sem is not None:
            send(src, dst, c_send, core_sem, span, other).start()

    hand_on(pack.at[span], model, 0, 0, p_recv.at[0], m_recv.at[0], cown_recv.at[0])
    own.start()
    for k in range(1, 16):
        to = span ^ k
        send(pack.at[to], rows.at[model, k], a_send, a_recv.at[k], to, model).start()
    own.wait()

    @pl.loop(1, 16)
    def _(k):
        block = rows.at[model, k]
        send(block, block, a_send, a_recv.at[k], span, model).wait_recv()
        hand_on(block, model, k, 0, p_recv.at[k], m_recv.at[k], cown_recv.at[k])

    @pl.loop(0, 64 + LAG)
    def _(n):
        @pl.when(n < 64)
        def _():
            t, k = n // 16, lax.rem(n, 16)
            odd = lax.rem(k, 2)
            mp = lax.rem(model + 30 - 2 * t, 16)
            mm = lax.rem(model + 2 + 2 * t, 16)

            @pl.when((t < 3) | (odd == 0))
            def _():
                block = rows.at[mp, k]
                send(block, block, c_send, p_recv.at[n], span, up).wait_recv()

                @pl.when(t < 2)
                def _():
                    hand_on(block, mp, k, 0, p_recv.at[n + 16], None, None)

                @pl.when((t == 2) & (odd == 0))
                def _():
                    hand_on(block, mp, k, 1, p_recv.at[n + 16], None, None)

                hand_on(block, mp, k, 0, None, None, cp_recv.at[n])

            @pl.when((t < 3) | (odd == 1))
            def _():
                block = rows.at[mm, k]
                send(block, block, c_send, m_recv.at[n], span, up).wait_recv()

                @pl.when(t < 2)
                def _():
                    hand_on(block, mm, k, 0, None, m_recv.at[n + 16], None)

                @pl.when((t == 2) & (odd == 1))
                def _():
                    hand_on(block, mm, k, 1, None, m_recv.at[n + 16], None)

                hand_on(block, mm, k, 0, None, None, cm_recv.at[n])

        @pl.when(n >= LAG)
        def _():
            i = n - LAG
            t, k = i // 16, lax.rem(i, 16)
            odd = lax.rem(k, 2)
            block = rows.at[other, k]

            @pl.when(t == 0)
            def _():
                send(block, block, c_send, cown_recv.at[k], span, other).wait_recv()

            @pl.when((t < 3) | (odd == 0))
            def _():
                send(block, block, c_send, cp_recv.at[i], span, other).wait_recv()

            @pl.when((t < 3) | (odd == 1))
            def _():
                send(block, block, c_send, cm_recv.at[i], span, other).wait_recv()

            side = 1 - 2 * lax.rem(z, 2)
            shift = jnp.where(t == 0, 0, jnp.where(t == 1, 4 - side, jnp.where(t == 2, 4 + side, 2)))
            pair = lax.rem(z // 2 + shift, 4)
            blocks = [rows[4 * pair + j, k] for j in range(4)]
            keys, rotary, values = tile_of(blocks, gain, wkt, wv, groups, wide)
            at = pl.multiple_of((span ^ k) * 512 + pair * 128, 128)
            keys_ref[:128, pl.ds(at, 128)] = keys
            keys_ref[128:, pl.ds(at, 128)] = rotary
            values_ref[pl.ds(at, 128), :] = values

    send(pack.at[pl.ds(0, 15)], rows.at[model, pl.ds(0, 15)], a_send, a_recv.at[0], span, other).wait_send()
    send(rows.at[pl.ds(0, 6)], rows.at[pl.ds(0, 6)], z_send.at[0], a_recv.at[0], span, other).wait_send()
    send(rows.at[0], rows.at[0], z_send.at[1], a_recv.at[0], span, other).wait_send()
    send(rows.at[pl.ds(0, 8)], rows.at[pl.ds(0, 8)], c_send, a_recv.at[0], span, other).wait_send()


def put_out(keys_ref, values_ref, keys_hbm, values_hbm, sems):
    copies = []
    for i in range(4):
        copies.append(
            pltpu.make_async_copy(
                keys_ref.at[pl.ds(48 * i, 48)], keys_hbm.at[pl.ds(48 * i, 48)], sems.at[i]
            )
        )
        copies.append(
            pltpu.make_async_copy(
                values_ref.at[pl.ds(2048 * i, 2048)],
                values_hbm.at[pl.ds(2048 * i, 2048)],
                sems.at[4 + i],
            )
        )
    for d in copies:
        d.start()
    for d in copies:
        d.wait()


def shards(latents, rotary_rows, latent_gain, key_up, value_up):
    any_space = pl.BlockSpec(memory_space=pl.ANY)
    vmem = pl.BlockSpec(memory_space=pltpu.VMEM)
    batch, wide, depth = latents.shape
    keys_shape = jax.ShapeDtypeStruct((192, 8192), jnp.bfloat16)
    values_shape = jax.ShapeDtypeStruct((8192, 128), jnp.bfloat16)
    dma, bf16 = pltpu.SemaphoreType.DMA, jnp.bfloat16
    tall = depth // LANES * wide + wide // 2
    keys, values = pl.pallas_call(
        exchange,
        out_shape=(keys_shape, values_shape),
        in_specs=[any_space] * 5,
        out_specs=(vmem, vmem),
        scratch_shapes=[
            pltpu.VMEM((batch, tall, LANES), bf16),
            pltpu.VMEM((16, 16, tall, LANES), bf16),
            pltpu.VMEM((batch, wide, 64), bf16),
            pltpu.VMEM((1, depth), jnp.float32),
            pltpu.VMEM((depth, 128), bf16),
            pltpu.VMEM((depth, 128), bf16),
            pltpu.VMEM((128, depth), bf16),
            dma((8,)), dma, dma, dma((2,)), dma,
            dma((16,)), dma((64,)), dma((64,)), dma((16,)), dma((64,)), dma((64,)),
        ],
        compiler_params=pltpu.CompilerParams(
            collective_id=0, has_side_effects=True, vmem_limit_bytes=24 * 1024 * 1024
        ),
        cost_estimate=pl.CostEstimate(flops=2 * 8192 * 512 * 256, bytes_accessed=1 << 20, transcendentals=0),
    )(
        latents,
        rotary_rows,
        latent_gain.reshape(1, depth),
        key_up.reshape(depth, 128),
        value_up.reshape(depth, 128),
    )
    keys, values = pl.pallas_call(
        put_out,
        out_shape=(keys_shape, values_shape),
        in_specs=[vmem, vmem],
        out_specs=(any_space, any_space),
        scratch_shapes=[dma((8,))],
    )(keys, values)
    return keys.reshape(1, 1, 192, 8192), values.reshape(1, 8192, 1, 128)


def solution(mesh):
    placed = (
        P(None, ("span", "model"), None),
        P(None, ("span", "model"), None),
        P(),
        P(None, "model", None),
        P(None, "model", None),
    )
    return jax.shard_map(
        shards,
        mesh=mesh,
        in_specs=placed,
        out_specs=(P("span", "model", None, None), P("span", None, "model", None)),
        check_vma=False,
    )
```

```python
import functools

import jax
import jax.numpy as jnp
from jax import lax
from jax.experimental import pallas as pl
from jax.experimental.pallas import tpu as pltpu
from jax.sharding import PartitionSpec as P

MESH = pl.DeviceIdType.MESH
LANES = 128
WIDE = 32
GROUPS = 4
DEPTH = GROUPS * LANES
TALL = GROUPS * WIDE + WIDE // 2
MASKS = (0, 1, 3, 4, 12, 5, 7, 13, 6, 14, 2, 15, 8, 9, 10, 11)
ARRIVALS = ((1,), (2, 3), (4, 5, 6, 7), (8, 9, 10, 11), (12, 13, 14, 15))


def normalized(rows, pair, slot, gain, xn, at):
    blocks = [rows[4 * pair + b, slot] for b in range(4)]
    x = [
        jnp.concatenate([b[g * WIDE : (g + 1) * WIDE] for b in blocks], axis=0).astype(jnp.float32)
        for g in range(GROUPS)
    ]
    squares = functools.reduce(lambda a, b: a + b, [v * v for v in x])
    scale = lax.rsqrt(jnp.sum(squares, axis=-1, keepdims=True) / DEPTH + 1e-06)
    for g in range(GROUPS):
        lanes = slice(g * LANES, (g + 1) * LANES)
        xn[at : at + LANES, lanes] = (x[g] * scale * gain[:, lanes]).astype(jnp.bfloat16)
    turned = []
    for b in blocks:
        packed = b[GROUPS * WIDE :].astype(jnp.float32)
        turned += [packed, pltpu.roll(packed, LANES // 2, 1)]
    return jnp.concatenate(turned, axis=0).astype(jnp.bfloat16)


def expand(rows, pair, slots, places, gain, w, xn, keys, values):
    rotary = [normalized(rows, pair, s, gain, xn, LANES * i) for i, s in enumerate(slots)]
    both = jnp.dot(xn[...], w[...], preferred_element_type=jnp.float32).astype(jnp.bfloat16)
    for i, at in enumerate(places):
        part = both[LANES * i : LANES * (i + 1)]
        values[pl.ds(at, LANES), :] = part[:, LANES:]
        keys[:LANES, pl.ds(at, LANES)] = part[:, :LANES].T
        keys[LANES:, pl.ds(at, LANES)] = rotary[i].T[: LANES // 2]


def place_of(source, pair):
    return pl.multiple_of(source * 512 + pair * LANES, LANES)


def mask_of(group, i):
    a, b, c, d = (MASKS[4 * g + i] for g in range(4))
    return jnp.where(group == 0, a, jnp.where(group == 1, b, jnp.where(group == 2, c, d)))


def exchange(
    lat_hbm, rot_hbm, gain_hbm, wk_hbm, wv_hbm,
    rows, keys, values, w, gain,
    pack, rot, xn,
    in_sems, a_send, z_send, c_send, a_recv, p_recv, m_recv, c_recv,
):
    span, model = lax.axis_index("span"), lax.axis_index("model")
    z, c = model // 2, lax.rem(model, 2)
    up = lax.rem(model + 2, 16)
    down = lax.rem(model + 14, 16)
    other = model + 1 - 2 * c

    barrier = pltpu.get_barrier_semaphore()
    for mask in MASKS[1:]:
        pl.semaphore_signal(barrier, inc=1, device_id=(span ^ mask, model), device_id_type=MESH)
    for m in (up, down, other):
        pl.semaphore_signal(barrier, inc=1, device_id=(span, m), device_id_type=MESH)

    pltpu.make_async_copy(rot_hbm, rot, in_sems.at[0]).start()
    for g in range(GROUPS):
        pltpu.make_async_copy(
            lat_hbm.at[:, :, pl.ds(g * LANES, LANES)],
            pack.at[:, pl.ds(g * WIDE, WIDE), :],
            in_sems.at[1],
        ).start()
    pltpu.make_async_copy(gain_hbm, gain, in_sems.at[2]).start()
    pltpu.make_async_copy(wk_hbm, w.at[:, pl.ds(0, LANES)], in_sems.at[3]).start()
    pltpu.make_async_copy(wv_hbm, w.at[:, pl.ds(LANES, LANES)], in_sems.at[3]).start()
    pltpu.make_async_copy(rot_hbm, rot, in_sems.at[0]).wait()
    half = WIDE // 2
    pack[:, GROUPS * WIDE :, :] = jnp.concatenate([rot[:, :half, :], rot[:, half:, :]], axis=-1)
    landed = pack.at[:, pl.ds(0, GROUPS * WIDE), :]
    pltpu.make_async_copy(landed, landed, in_sems.at[1]).wait()
    pl.semaphore_wait(barrier, 18)

    def send(src, dst, send_sem, recv_sem, s, m):
        return pltpu.make_async_remote_copy(
            src_ref=src, dst_ref=dst, send_sem=send_sem, recv_sem=recv_sem,
            device_id=(s, m), device_id_type=MESH,
        )

    def arrived(count, sem):
        piece = rows.at[0, pl.ds(0, count)]
        send(piece, piece, c_send, sem, span, other).wait_recv()

    def upward(src, dst, zs, sem):
        send(src, dst, z_send.at[zs], sem, span, up).start()

    def downward(src, dst, zs, sem):
        send(src, dst, z_send.at[zs], sem, span, down).start()

    def across(src, dst, sem):
        send(src, dst, c_send, sem, span, other).start()

    first, first_at = pack.at[span], rows.at[model, 0]
    upward(first, first_at, 0, p_recv.at[0])
    downward(first, first_at, 0, m_recv.at[0])
    for group, slots in enumerate(ARRIVALS):
        for slot in slots:
            to = span ^ MASKS[slot]
            send(pack.at[to], rows.at[model, slot], a_send, a_recv.at[group], to, model).start()
    across(first, first_at, c_recv.at[0])
    rows[model, 0] = pack[span]
    pltpu.make_async_copy(gain_hbm, gain, in_sems.at[2]).wait()
    pltpu.make_async_copy(w, w, in_sems.at[3]).wait()

    for group, slots in enumerate(ARRIVALS):
        arrived(len(slots), a_recv.at[group])
        piece, j = rows.at[model, pl.ds(slots[0], len(slots))], slots[0] // 4
        upward(piece, piece, 0, p_recv.at[j])
        downward(piece, piece, 0, m_recv.at[j])
        across(piece, piece, c_recv.at[j])

    side = 1 - 2 * lax.rem(z, 2)

    @pl.loop(0, 17)
    def _(n):
        @pl.when(n < 16)
        def _():
            t, j = n // 4, lax.rem(n, 4)
            mp = lax.rem(model + 30 - 2 * t, 16)
            mm = lax.rem(model + 2 + 2 * t, 16)
            from_below, from_above = rows.at[mp, pl.ds(4 * j, 4)], rows.at[mm, pl.ds(4 * j, 4)]
            low, high = rows.at[mp, pl.ds(4 * j, 2)], rows.at[mm, pl.ds(4 * j + 2, 2)]

            @pl.when(t < 3)
            def _():
                arrived(4, p_recv.at[n])

                @pl.when(t < 2)
                def _():
                    upward(from_below, from_below, 0, p_recv.at[n + 4])

                @pl.when(t == 2)
                def _():
                    upward(low, low, 1, p_recv.at[n + 4])

                arrived(4, m_recv.at[n])

                @pl.when(t < 2)
                def _():
                    downward(from_above, from_above, 0, m_recv.at[n + 4])

                @pl.when(t == 2)
                def _():
                    downward(high, high, 1, m_recv.at[n + 4])

                across(from_below, from_below, c_recv.at[n])
                across(from_above, from_above, c_recv.at[n])

            @pl.when(t == 3)
            def _():
                arrived(2, p_recv.at[n])
                across(low, low, c_recv.at[n])
                arrived(2, m_recv.at[n])
                across(high, high, c_recv.at[n])

        @pl.when(n >= 1)
        def _():
            i = n - 1
            t, j = i // 4, lax.rem(i, 4)

            @pl.when(t == 0)
            def _():
                arrived(12, c_recv.at[i])

            @pl.when((t == 1) | (t == 2))
            def _():
                arrived(8, c_recv.at[i])

            @pl.when(t == 3)
            def _():
                arrived(4, c_recv.at[i])

            @pl.when(i < 15)
            def _():
                shift = jnp.where(
                    t == 0, 0, jnp.where(t == 1, 4 - side, jnp.where(t == 2, 4 + side, 2))
                )
                pair = lax.rem(z // 2 + shift, 4)
                expand(
                    rows, pair, [4 * j + s for s in range(4)],
                    [place_of(span ^ mask_of(j, s), pair) for s in range(4)],
                    gain, w, xn, keys, values,
                )

    send(pack.at[pl.ds(0, 15)], rows.at[0, pl.ds(0, 15)], a_send, a_recv.at[0], span, other).wait_send()
    send(rows.at[pl.ds(0, 6)], rows.at[pl.ds(0, 6)], z_send.at[0], a_recv.at[0], span, other).wait_send()
    send(rows.at[0], rows.at[0], z_send.at[1], a_recv.at[0], span, other).wait_send()
    send(rows.at[pl.ds(0, 8)], rows.at[pl.ds(0, 8)], c_send, a_recv.at[0], span, other).wait_send()


def finish(rows, keys, values, w, gain, keys_hbm, values_hbm, xn, last_keys, last_values, sems):
    span, model = lax.axis_index("span"), lax.axis_index("model")
    last = (span // 4) ^ 2
    pair = lax.rem(model // 4 + 2, 4)
    places = [place_of(span ^ mask, pair) for mask in MASKS[12:]]

    def leave(keys_from, k, values_from, v):
        pltpu.make_async_copy(keys_from, keys_hbm.at[:, k], sems.at[0]).start()
        pltpu.make_async_copy(values_from, values_hbm.at[v], sems.at[1]).start()

    for i in range(1, 4):
        at = pl.ds(pl.multiple_of((last ^ i) * 2048, 2048), 2048)
        leave(keys.at[:, at], at, values.at[at], at)
    for i in range(4):
        for other in range(1, 4):
            at = pl.ds(place_of(last * 4 + i, lax.rem(pair + other, 4)), LANES)
            leave(keys.at[:, at], at, values.at[at], at)
    expand(
        rows, pair, range(12, 16), [LANES * i for i in range(4)], gain, w, xn, last_keys, last_values
    )
    for i in range(4):
        here, at = pl.ds(LANES * i, LANES), pl.ds(places[i], LANES)
        leave(last_keys.at[:, here], at, last_values.at[here], at)
    pltpu.make_async_copy(keys, keys_hbm, sems.at[0]).wait()
    pltpu.make_async_copy(values, values_hbm, sems.at[1]).wait()


def shards(latents, rotary_rows, latent_gain, key_up, value_up):
    hbm = pl.BlockSpec(memory_space=pltpu.HBM)
    vmem = pl.BlockSpec(memory_space=pltpu.VMEM)
    dma, bf16, f32 = pltpu.SemaphoreType.DMA, jnp.bfloat16, jnp.float32
    keys_shape = jax.ShapeDtypeStruct((192, 8192), bf16)
    values_shape = jax.ShapeDtypeStruct((8192, 128), bf16)
    ready = pl.pallas_call(
        exchange,
        out_shape=(
            jax.ShapeDtypeStruct((16, 16, TALL, LANES), bf16),
            keys_shape,
            values_shape,
            jax.ShapeDtypeStruct((DEPTH, 2 * LANES), bf16),
            jax.ShapeDtypeStruct((1, DEPTH), f32),
        ),
        in_specs=[hbm] * 5,
        out_specs=(vmem,) * 5,
        scratch_shapes=[
            pltpu.VMEM((16, TALL, LANES), bf16),
            pltpu.VMEM((16, WIDE, 64), bf16),
            pltpu.VMEM((512, DEPTH), bf16),
            dma((4,)), dma, dma((2,)), dma,
            dma((5,)), dma((16,)), dma((16,)), dma((16,)),
        ],
        compiler_params=pltpu.CompilerParams(
            collective_id=0, has_side_effects=True, vmem_limit_bytes=8 * 1024 * 1024
        ),
        cost_estimate=pl.CostEstimate(flops=2 * 8192 * 512 * 256, bytes_accessed=1 << 20, transcendentals=0),
    )(
        *(
            pltpu.with_memory_space_constraint(a, pltpu.HBM)
            for a in (
                latents,
                rotary_rows,
                latent_gain.reshape(1, DEPTH),
                key_up.reshape(DEPTH, LANES),
                value_up.reshape(DEPTH, LANES),
            )
        )
    )
    keys, values = pl.pallas_call(
        finish,
        out_shape=(keys_shape, values_shape),
        in_specs=[vmem] * 5,
        out_specs=(hbm, hbm),
        scratch_shapes=[
            pltpu.VMEM((512, DEPTH), bf16),
            pltpu.VMEM((192, 512), bf16),
            pltpu.VMEM((512, LANES), bf16),
            dma((2,)),
        ],
        compiler_params=pltpu.CompilerParams(vmem_limit_bytes=4 * 1024 * 1024),
    )(*ready)
    return keys.reshape(1, 1, 192, 8192), values.reshape(1, 8192, 1, 128)


def solution(mesh):
    placed = (
        P(None, ("span", "model"), None),
        P(None, ("span", "model"), None),
        P(),
        P(None, "model", None),
        P(None, "model", None),
    )
    return jax.shard_map(
        shards,
        mesh=mesh,
        in_specs=placed,
        out_specs=(P("span", "model", None, None), P("span", None, "model", None)),
        check_vma=False,
    )
```

```python
import functools

import jax
import jax.numpy as jnp
from jax import lax
from jax.experimental import pallas as pl
from jax.experimental.pallas import tpu as pltpu
from jax.sharding import PartitionSpec as P

MESH = pl.DeviceIdType.MESH
LANES = 128
WIDE = 32
GROUPS = 4
DEPTH = GROUPS * LANES
TALL = GROUPS * WIDE + WIDE // 2
MASKS = (0, 1, 3, 4, 12, 5, 7, 13, 2, 15, 6, 14, 8, 9, 10, 11)
NEAR, MIDDLE, FAR = (1, 2, 3, 4), (5, 6, 7), (8, 9, 12, 10, 11, 13, 15, 14)
RISING = (2, 2, 1, 1)


def hops(mask):
    return (0, 1, 2, 1)[mask % 4] + (0, 1, 2, 1)[mask // 4]


def normalized(rows, pair, slot, gain, xn, at):
    blocks = [rows[4 * pair + b, slot] for b in range(4)]
    x = [
        jnp.concatenate([b[g * WIDE : (g + 1) * WIDE] for b in blocks], axis=0).astype(jnp.float32)
        for g in range(GROUPS)
    ]
    squares = functools.reduce(lambda a, b: a + b, [v * v for v in x])
    scale = lax.rsqrt(jnp.sum(squares, axis=-1, keepdims=True) / DEPTH + 1e-06)
    for g in range(GROUPS):
        lanes = slice(g * LANES, (g + 1) * LANES)
        xn[at : at + LANES, lanes] = (x[g] * scale * gain[:, lanes]).astype(jnp.bfloat16)
    turned = []
    for b in blocks:
        packed = b[GROUPS * WIDE :].astype(jnp.float32)
        turned += [packed, pltpu.roll(packed, LANES // 2, 1)]
    return jnp.concatenate(turned, axis=0).astype(jnp.bfloat16)


def expand(rows, pair, slots, places, gain, w, xn, keys, values):
    rotary = [normalized(rows, pair, s, gain, xn, LANES * i) for i, s in enumerate(slots)]
    both = jnp.dot(xn[...], w[...], preferred_element_type=jnp.float32).astype(jnp.bfloat16)
    for i, at in enumerate(places):
        part = both[LANES * i : LANES * (i + 1)]
        values[pl.ds(at, LANES), :] = part[:, LANES:]
        keys[:LANES, pl.ds(at, LANES)] = part[:, :LANES].T
        keys[LANES:, pl.ds(at, LANES)] = rotary[i].T[: LANES // 2]


def place_of(source, pair):
    return pl.multiple_of(source * 512 + pair * LANES, LANES)


def mask_of(group, i):
    a, b, c, d = (MASKS[4 * g + i] for g in range(4))
    return jnp.where(group == 0, a, jnp.where(group == 1, b, jnp.where(group == 2, c, d)))


def exchange(
    lat_hbm, rot_hbm, gain_hbm, wk_hbm, wv_hbm,
    rows, keys, values, w, gain,
    pack, rot, xn, stage_up, stage_down,
    in_sems, a_send, r_send, z_send, c_send, a_recv, p_recv, m_recv, c_recv, stage_recv, token,
):
    span, model = lax.axis_index("span"), lax.axis_index("model")
    z, c = model // 2, lax.rem(model, 2)
    up = lax.rem(model + 2, 16)
    down = lax.rem(model + 14, 16)
    other = model + 1 - 2 * c

    barrier = pltpu.get_barrier_semaphore()
    for m in (up, down, other):
        pl.semaphore_signal(barrier, inc=1, device_id=(span, m), device_id_type=MESH)
    near = [span ^ MASKS[slot] for slot in NEAR]
    for s in near:
        pl.semaphore_signal(barrier, inc=1, device_id=(s, model), device_id_type=MESH)

    pltpu.make_async_copy(rot_hbm, rot, in_sems.at[0]).start()
    for g in range(GROUPS):
        pltpu.make_async_copy(
            lat_hbm.at[:, :, pl.ds(g * LANES, LANES)],
            pack.at[:, pl.ds(g * WIDE, WIDE), :],
            in_sems.at[1],
        ).start()
    pltpu.make_async_copy(gain_hbm, gain, in_sems.at[2]).start()
    pltpu.make_async_copy(wk_hbm, w.at[:, pl.ds(0, LANES)], in_sems.at[3]).start()
    pltpu.make_async_copy(wv_hbm, w.at[:, pl.ds(LANES, LANES)], in_sems.at[3]).start()
    pltpu.make_async_copy(rot_hbm, rot, in_sems.at[0]).wait()
    half = WIDE // 2
    pack[:, GROUPS * WIDE :, :] = jnp.concatenate([rot[:, :half, :], rot[:, half:, :]], axis=-1)
    landed = pack.at[:, pl.ds(0, GROUPS * WIDE), :]
    pltpu.make_async_copy(landed, landed, in_sems.at[1]).wait()
    pl.semaphore_wait(barrier, 7)

    def send(src, dst, send_sem, recv_sem, s, m):
        return pltpu.make_async_remote_copy(
            src_ref=src, dst_ref=dst, send_sem=send_sem, recv_sem=recv_sem,
            device_id=(s, m), device_id_type=MESH,
        )

    def arrived(count, sem):
        piece = rows.at[0, pl.ds(0, count)]
        send(piece, piece, c_send, sem, span, other).wait_recv()

    def upward(src, dst, zs, sem):
        send(src, dst, z_send.at[zs], sem, span, up).start()

    def downward(src, dst, zs, sem):
        send(src, dst, z_send.at[zs], sem, span, down).start()

    def across(src, dst, sem):
        send(src, dst, c_send, sem, span, other).start()

    def spread(slot, sem):
        to = span ^ MASKS[slot]
        send(pack.at[to], rows.at[model, slot], a_send, a_recv.at[sem], to, model).start()

    first, first_at = pack.at[span], rows.at[model, 0]
    upward(first, first_at, 0, p_recv.at[0])
    downward(first, first_at, 0, m_recv.at[0])
    for slot in NEAR + MIDDLE:
        src, sem = pack.at[span ^ MASKS[slot]], slot // 5
        upward(src, stage_up.at[slot - 1], 0, stage_recv.at[sem])
        downward(src, stage_down.at[slot - 1], 0, stage_recv.at[2 + sem])
    for slot in NEAR:
        spread(slot, 0)

    for far in range(2, 5):
        for s in near:
            pl.semaphore_signal(token.at[far - 2], inc=1, device_id=(s, model), device_id_type=MESH)
        if far == 2:
            across(first, first_at, c_recv.at[0])
            rows[model, 0] = pack[span]
        pl.semaphore_wait(token.at[far - 2], 4)
        for i, slot in enumerate(FAR):
            if hops(MASKS[slot]) == far:
                spread(slot, 2 + i)
    for slot in MIDDLE:
        spread(slot, 1)

    def relay(slots, stage, sem, origin, recv):
        piece = rows.at[origin, pl.ds(slots[0], len(slots))]
        part = stage.at[pl.ds(slots[0] - 1, len(slots))]
        send(part, piece, r_send, stage_recv.at[sem], span, up).wait_recv()
        for slot in slots:
            send(
                stage.at[slot - 1], rows.at[origin, slot], r_send, recv.at[slot // 4],
                span ^ MASKS[slot], model,
            ).start()

    for i, slot in enumerate(FAR):
        arrived(1, a_recv.at[2 + i])
        piece = rows.at[model, slot]
        upward(piece, piece, 0, p_recv.at[slot // 4])
        downward(piece, piece, 0, m_recv.at[slot // 4])
        if i == 2:
            relay(NEAR, stage_up, 0, down, p_recv)
            relay(NEAR, stage_down, 2, up, m_recv)
        if i == 6:
            relay(MIDDLE, stage_up, 1, down, p_recv)
            relay(MIDDLE, stage_down, 3, up, m_recv)
    arrived(4, a_recv.at[0])
    arrived(3, a_recv.at[1])
    for start, count in ((1, 3), (4, 4), (8, 4), (12, 4)):
        piece = rows.at[model, pl.ds(start, count)]
        across(piece, piece, c_recv.at[start // 4])
    pltpu.make_async_copy(gain_hbm, gain, in_sems.at[2]).wait()
    pltpu.make_async_copy(w, w, in_sems.at[3]).wait()

    side = 1 - 2 * lax.rem(z, 2)

    def tile(t, j):
        shift = jnp.where(t == 0, 0, jnp.where(t == 1, 4 - side, jnp.where(t == 2, 4 + side, 2)))
        pair = lax.rem(z // 2 + shift, 4)
        expand(
            rows, pair, [4 * j + s for s in range(4)],
            [place_of(span ^ mask_of(j, s), pair) for s in range(4)],
            gain, w, xn, keys, values,
        )

    @pl.loop(0, 12)
    def _(n):
        t, j = n // 4, lax.rem(n, 4)
        mp = lax.rem(model + 30 - 2 * t, 16)
        mm = lax.rem(model + 2 + 2 * t, 16)
        from_below, from_above = rows.at[mp, pl.ds(4 * j, 4)], rows.at[mm, pl.ds(4 * j, 4)]
        arrived(4, p_recv.at[n])

        @pl.when(t < 2)
        def _():
            upward(from_below, from_below, 0, p_recv.at[n + 4])

        for part, count in enumerate(RISING):

            @pl.when(n == 8 + part)
            def _():
                piece = rows.at[mp, pl.ds(4 * part, count)]
                upward(piece, piece, 1, p_recv.at[12 + part])

        arrived(4, m_recv.at[n])

        @pl.when(t < 2)
        def _():
            downward(from_above, from_above, 0, m_recv.at[n + 4])

        for part, count in enumerate(RISING):

            @pl.when(n == 8 + part)
            def _():
                piece = rows.at[mm, pl.ds(4 * part + count, 4 - count)]
                downward(piece, piece, 1, m_recv.at[12 + part])

        across(from_below, from_below, c_recv.at[n])
        across(from_above, from_above, c_recv.at[n])

        @pl.when(n >= 1)
        def _():
            i = n - 1

            @pl.when(i < 4)
            def _():
                arrived(12, c_recv.at[i])

            @pl.when(i >= 4)
            def _():
                arrived(8, c_recv.at[i])

            tile(i // 4, lax.rem(i, 4))

    opposite = lax.rem(model + 8, 16)
    for part, count in enumerate(RISING):
        low = rows.at[opposite, pl.ds(4 * part, count)]
        high = rows.at[opposite, pl.ds(4 * part + count, 4 - count)]
        arrived(count, p_recv.at[12 + part])
        across(low, low, c_recv.at[12 + part])
        arrived(4 - count, m_recv.at[12 + part])
        across(high, high, c_recv.at[12 + part])
        if part == 0:
            arrived(8, c_recv.at[11])
            tile(2, 3)
        else:
            arrived(4, c_recv.at[11 + part])
            tile(3, part - 1)
    arrived(4, c_recv.at[15])

    send(pack.at[pl.ds(0, 15)], rows.at[0, pl.ds(0, 15)], a_send, a_recv.at[0], span, other).wait_send()
    send(rows.at[0, pl.ds(0, 14)], rows.at[0, pl.ds(0, 14)], r_send, a_recv.at[0], span, other).wait_send()
    send(rows.at[pl.ds(0, 6)], rows.at[pl.ds(0, 6)], z_send.at[0], a_recv.at[0], span, other).wait_send()
    send(rows.at[0], rows.at[0], z_send.at[1], a_recv.at[0], span, other).wait_send()
    send(rows.at[pl.ds(0, 8)], rows.at[pl.ds(0, 8)], c_send, a_recv.at[0], span, other).wait_send()


def finish(rows, keys, values, w, gain, keys_hbm, values_hbm, xn, last_keys, last_values, sems):
    span, model = lax.axis_index("span"), lax.axis_index("model")
    last = (span // 4) ^ 2
    pair = lax.rem(model // 4 + 2, 4)
    places = [place_of(span ^ mask, pair) for mask in MASKS[12:]]

    def leave(keys_from, k, values_from, v):
        pltpu.make_async_copy(keys_from, keys_hbm.at[:, k], sems.at[0]).start()
        pltpu.make_async_copy(values_from, values_hbm.at[v], sems.at[1]).start()

    for i in range(1, 4):
        at = pl.ds(pl.multiple_of((last ^ i) * 2048, 2048), 2048)
        leave(keys.at[:, at], at, values.at[at], at)
    for i in range(4):
        for other in range(1, 4):
            at = pl.ds(place_of(last * 4 + i, lax.rem(pair + other, 4)), LANES)
            leave(keys.at[:, at], at, values.at[at], at)
    expand(
        rows, pair, range(12, 16), [LANES * i for i in range(4)], gain, w, xn, last_keys, last_values
    )
    for i in range(4):
        here, at = pl.ds(LANES * i, LANES), pl.ds(places[i], LANES)
        leave(last_keys.at[:, here], at, last_values.at[here], at)
    pltpu.make_async_copy(keys, keys_hbm, sems.at[0]).wait()
    pltpu.make_async_copy(values, values_hbm, sems.at[1]).wait()


def shards(latents, rotary_rows, latent_gain, key_up, value_up):
    hbm = pl.BlockSpec(memory_space=pltpu.HBM)
    vmem = pl.BlockSpec(memory_space=pltpu.VMEM)
    dma, bf16, f32 = pltpu.SemaphoreType.DMA, jnp.bfloat16, jnp.float32
    keys_shape = jax.ShapeDtypeStruct((192, 8192), bf16)
    values_shape = jax.ShapeDtypeStruct((8192, 128), bf16)
    ready = pl.pallas_call(
        exchange,
        out_shape=(
            jax.ShapeDtypeStruct((16, 16, TALL, LANES), bf16),
            keys_shape,
            values_shape,
            jax.ShapeDtypeStruct((DEPTH, 2 * LANES), bf16),
            jax.ShapeDtypeStruct((1, DEPTH), f32),
        ),
        in_specs=[hbm] * 5,
        out_specs=(vmem,) * 5,
        scratch_shapes=[
            pltpu.VMEM((16, TALL, LANES), bf16),
            pltpu.VMEM((16, WIDE, 64), bf16),
            pltpu.VMEM((512, DEPTH), bf16),
            pltpu.VMEM((7, TALL, LANES), bf16),
            pltpu.VMEM((7, TALL, LANES), bf16),
            dma((4,)), dma, dma, dma((2,)), dma,
            dma((10,)), dma((16,)), dma((16,)), dma((16,)), dma((4,)),
            pltpu.SemaphoreType.REGULAR((3,)),
        ],
        compiler_params=pltpu.CompilerParams(
            collective_id=0, has_side_effects=True, vmem_limit_bytes=8 * 1024 * 1024
        ),
        cost_estimate=pl.CostEstimate(flops=2 * 8192 * 512 * 256, bytes_accessed=1 << 20, transcendentals=0),
    )(
        *(
            pltpu.with_memory_space_constraint(a, pltpu.HBM)
            for a in (
                latents,
                rotary_rows,
                latent_gain.reshape(1, DEPTH),
                key_up.reshape(DEPTH, LANES),
                value_up.reshape(DEPTH, LANES),
            )
        )
    )
    keys, values = pl.pallas_call(
        finish,
        out_shape=(keys_shape, values_shape),
        in_specs=[vmem] * 5,
        out_specs=(hbm, hbm),
        scratch_shapes=[
            pltpu.VMEM((512, DEPTH), bf16),
            pltpu.VMEM((192, 512), bf16),
            pltpu.VMEM((512, LANES), bf16),
            dma((2,)),
        ],
        compiler_params=pltpu.CompilerParams(vmem_limit_bytes=4 * 1024 * 1024),
    )(*ready)
    return keys.reshape(1, 1, 192, 8192), values.reshape(1, 8192, 1, 128)


def solution(mesh):
    placed = (
        P(None, ("span", "model"), None),
        P(None, ("span", "model"), None),
        P(),
        P(None, "model", None),
        P(None, "model", None),
    )
    return jax.shard_map(
        shards,
        mesh=mesh,
        in_specs=placed,
        out_specs=(P("span", "model", None, None), P("span", None, "model", None)),
        check_vma=False,
    )
```

```python
import functools

import jax
import jax.numpy as jnp
from jax import lax
from jax.experimental import pallas as pl
from jax.experimental.pallas import tpu as pltpu
from jax.sharding import PartitionSpec as P

MESH = pl.DeviceIdType.MESH
LANES = 128
WIDE = 32
GROUPS = 4
DEPTH = GROUPS * LANES
TALL = GROUPS * WIDE + WIDE // 2
MASKS = (0, 1, 3, 4, 12, 5, 7, 13, 2, 15, 6, 14, 8, 9, 10, 11)
NEAR, MIDDLE, FAR = (1, 2, 3, 4), (5, 6, 7, 8, 9, 12), (10, 11, 13, 14, 15)
RISING = (2, 2, 1, 1)


def normalized(rows, pair, slot, gain, xn, at):
    blocks = [rows[4 * pair + b, slot] for b in range(4)]
    x = [
        jnp.concatenate([b[g * WIDE : (g + 1) * WIDE] for b in blocks], axis=0).astype(jnp.float32)
        for g in range(GROUPS)
    ]
    squares = functools.reduce(lambda a, b: a + b, [v * v for v in x])
    scale = lax.rsqrt(jnp.sum(squares, axis=-1, keepdims=True) / DEPTH + 1e-06)
    for g in range(GROUPS):
        lanes = slice(g * LANES, (g + 1) * LANES)
        xn[at : at + LANES, lanes] = (x[g] * scale * gain[:, lanes]).astype(jnp.bfloat16)
    turned = []
    for b in blocks:
        packed = b[GROUPS * WIDE :].astype(jnp.float32)
        turned += [packed, pltpu.roll(packed, LANES // 2, 1)]
    return jnp.concatenate(turned, axis=0).astype(jnp.bfloat16)


def expand(rows, pair, slots, places, gain, w, xn, keys, values):
    rotary = [normalized(rows, pair, s, gain, xn, LANES * i) for i, s in enumerate(slots)]
    both = jnp.dot(xn[...], w[...], preferred_element_type=jnp.float32).astype(jnp.bfloat16)
    for i, at in enumerate(places):
        part = both[LANES * i : LANES * (i + 1)]
        values[pl.ds(at, LANES), :] = part[:, LANES:]
        keys[:LANES, pl.ds(at, LANES)] = part[:, :LANES].T
        keys[LANES:, pl.ds(at, LANES)] = rotary[i].T[: LANES // 2]


def place_of(source, pair):
    return pl.multiple_of(source * 512 + pair * LANES, LANES)


def mask_of(group, i):
    a, b, c, d = (MASKS[4 * g + i] for g in range(4))
    return jnp.where(group == 0, a, jnp.where(group == 1, b, jnp.where(group == 2, c, d)))


def exchange(
    lat_hbm, rot_hbm, gain_hbm, wk_hbm, wv_hbm,
    rows, keys, values, w, gain,
    pack, rot, xn, stage_up, stage_down,
    in_sems, a_send, r_send, z_send, c_send, a_recv, p_recv, m_recv, c_recv, stage_recv, token,
):
    span, model = lax.axis_index("span"), lax.axis_index("model")
    z, c = model // 2, lax.rem(model, 2)
    up = lax.rem(model + 2, 16)
    down = lax.rem(model + 14, 16)
    other = model + 1 - 2 * c

    barrier = pltpu.get_barrier_semaphore()
    for m in (up, down, other):
        pl.semaphore_signal(barrier, inc=1, device_id=(span, m), device_id_type=MESH)
    near = [span ^ MASKS[slot] for slot in NEAR]
    for s in near:
        pl.semaphore_signal(barrier, inc=1, device_id=(s, model), device_id_type=MESH)

    pltpu.make_async_copy(rot_hbm, rot, in_sems.at[0]).start()
    for g in range(GROUPS):
        pltpu.make_async_copy(
            lat_hbm.at[:, :, pl.ds(g * LANES, LANES)],
            pack.at[:, pl.ds(g * WIDE, WIDE), :],
            in_sems.at[1],
        ).start()
    pltpu.make_async_copy(gain_hbm, gain, in_sems.at[2]).start()
    pltpu.make_async_copy(wk_hbm, w.at[:, pl.ds(0, LANES)], in_sems.at[3]).start()
    pltpu.make_async_copy(wv_hbm, w.at[:, pl.ds(LANES, LANES)], in_sems.at[3]).start()
    pltpu.make_async_copy(rot_hbm, rot, in_sems.at[0]).wait()
    half = WIDE // 2
    pack[:, GROUPS * WIDE :, :] = jnp.concatenate([rot[:, :half, :], rot[:, half:, :]], axis=-1)
    landed = pack.at[:, pl.ds(0, GROUPS * WIDE), :]
    pltpu.make_async_copy(landed, landed, in_sems.at[1]).wait()
    pl.semaphore_wait(barrier, 7)

    def send(src, dst, send_sem, recv_sem, s, m):
        return pltpu.make_async_remote_copy(
            src_ref=src, dst_ref=dst, send_sem=send_sem, recv_sem=recv_sem,
            device_id=(s, m), device_id_type=MESH,
        )

    def arrived(count, sem):
        piece = rows.at[0, pl.ds(0, count)]
        send(piece, piece, c_send, sem, span, other).wait_recv()

    def upward(src, dst, zs, sem):
        send(src, dst, z_send.at[zs], sem, span, up).start()

    def downward(src, dst, zs, sem):
        send(src, dst, z_send.at[zs], sem, span, down).start()

    def across(src, dst, sem):
        send(src, dst, c_send, sem, span, other).start()

    def spread(slot, sem):
        to = span ^ MASKS[slot]
        send(pack.at[to], rows.at[model, slot], a_send, a_recv.at[sem], to, model).start()

    def onward(slot, sem):
        arrived(1, a_recv.at[sem])
        piece = rows.at[model, slot]
        upward(piece, piece, 0, p_recv.at[slot // 4])
        downward(piece, piece, 0, m_recv.at[slot // 4])

    def tell(turn):
        for s in near:
            pl.semaphore_signal(token.at[turn], inc=1, device_id=(s, model), device_id_type=MESH)

    first, first_at = pack.at[span], rows.at[model, 0]
    upward(first, first_at, 0, p_recv.at[0])
    downward(first, first_at, 0, m_recv.at[0])
    for i, slot in enumerate(NEAR):
        spread(slot, i)
    tell(0)
    for i, slot in enumerate(FAR):
        src = pack.at[span ^ MASKS[slot]]
        upward(src, stage_up.at[i], 0, stage_recv.at[0])
        downward(src, stage_down.at[i], 0, stage_recv.at[1])
    across(first, first_at, c_recv.at[0])
    rows[model, 0] = pack[span]
    pl.semaphore_wait(token.at[0], 4)
    for i, slot in enumerate(MIDDLE):
        spread(slot, 4 + i)
    tell(1)
    for i, slot in enumerate(NEAR):
        onward(slot, i)
    pl.semaphore_wait(token.at[1], 4)
    tell(2)
    for i, slot in enumerate(MIDDLE[:2]):
        onward(slot, 4 + i)
    pl.semaphore_wait(token.at[2], 4)
    for i, slot in enumerate(MIDDLE[2:]):
        onward(slot, 6 + i)

    for stage, sem, origin, recv in ((stage_up, 0, down, p_recv), (stage_down, 1, up, m_recv)):
        send(stage, stage, r_send, stage_recv.at[sem], span, up).wait_recv()
        for i, slot in enumerate(FAR):
            send(
                stage.at[i], rows.at[origin, slot], r_send, recv.at[slot // 4],
                span ^ MASKS[slot], model,
            ).start()
    for slot in FAR:
        spread(slot, 10)
    for start, count in ((1, 3), (4, 4), (8, 2), (12, 1)):
        piece = rows.at[model, pl.ds(start, count)]
        across(piece, piece, c_recv.at[start // 4])
    pltpu.make_async_copy(gain_hbm, gain, in_sems.at[2]).wait()
    pltpu.make_async_copy(w, w, in_sems.at[3]).wait()

    side = 1 - 2 * lax.rem(z, 2)

    def tile(t, j):
        shift = jnp.where(t == 0, 0, jnp.where(t == 1, 4 - side, jnp.where(t == 2, 4 + side, 2)))
        pair = lax.rem(z // 2 + shift, 4)
        expand(
            rows, pair, [4 * j + s for s in range(4)],
            [place_of(span ^ mask_of(j, s), pair) for s in range(4)],
            gain, w, xn, keys, values,
        )

    @pl.loop(0, 12)
    def _(n):
        t, j = n // 4, lax.rem(n, 4)
        mp = lax.rem(model + 30 - 2 * t, 16)
        mm = lax.rem(model + 2 + 2 * t, 16)
        from_below, from_above = rows.at[mp, pl.ds(4 * j, 4)], rows.at[mm, pl.ds(4 * j, 4)]
        arrived(4, p_recv.at[n])

        @pl.when(t < 2)
        def _():
            upward(from_below, from_below, 0, p_recv.at[n + 4])

        for part, count in enumerate(RISING):

            @pl.when(n == 8 + part)
            def _():
                piece = rows.at[mp, pl.ds(4 * part, count)]
                upward(piece, piece, 1, p_recv.at[12 + part])

        arrived(4, m_recv.at[n])

        @pl.when(t < 2)
        def _():
            downward(from_above, from_above, 0, m_recv.at[n + 4])

        for part, count in enumerate(RISING):

            @pl.when(n == 8 + part)
            def _():
                piece = rows.at[mm, pl.ds(4 * part + count, 4 - count)]
                downward(piece, piece, 1, m_recv.at[12 + part])

        @pl.when(n == 2)
        def _():
            arrived(5, a_recv.at[10])
            for start, count in ((10, 2), (13, 3)):
                piece = rows.at[model, pl.ds(start, count)]
                across(piece, piece, c_recv.at[start // 4])

        across(from_below, from_below, c_recv.at[n])
        across(from_above, from_above, c_recv.at[n])

        @pl.when(n >= 1)
        def _():
            i = n - 1

            @pl.when(i < 4)
            def _():
                arrived(12, c_recv.at[i])

            @pl.when(i >= 4)
            def _():
                arrived(8, c_recv.at[i])

            tile(i // 4, lax.rem(i, 4))

    opposite = lax.rem(model + 8, 16)
    for part, count in enumerate(RISING):
        low = rows.at[opposite, pl.ds(4 * part, count)]
        high = rows.at[opposite, pl.ds(4 * part + count, 4 - count)]
        arrived(count, p_recv.at[12 + part])
        across(low, low, c_recv.at[12 + part])
        arrived(4 - count, m_recv.at[12 + part])
        across(high, high, c_recv.at[12 + part])
        if part == 0:
            arrived(8, c_recv.at[11])
            tile(2, 3)
        else:
            arrived(4, c_recv.at[11 + part])
            tile(3, part - 1)
    arrived(4, c_recv.at[15])

    send(pack.at[pl.ds(0, 15)], rows.at[0, pl.ds(0, 15)], a_send, a_recv.at[0], span, other).wait_send()
    send(rows.at[0, pl.ds(0, 10)], rows.at[0, pl.ds(0, 10)], r_send, a_recv.at[0], span, other).wait_send()
    send(rows.at[pl.ds(0, 6)], rows.at[pl.ds(0, 6)], z_send.at[0], a_recv.at[0], span, other).wait_send()
    send(rows.at[0], rows.at[0], z_send.at[1], a_recv.at[0], span, other).wait_send()
    send(rows.at[pl.ds(0, 8)], rows.at[pl.ds(0, 8)], c_send, a_recv.at[0], span, other).wait_send()


def finish(rows, keys, values, w, gain, keys_hbm, values_hbm, xn, last_keys, last_values, sems):
    span, model = lax.axis_index("span"), lax.axis_index("model")
    last = (span // 4) ^ 2
    pair = lax.rem(model // 4 + 2, 4)
    places = [place_of(span ^ mask, pair) for mask in MASKS[12:]]

    def leave(keys_from, k, values_from, v):
        pltpu.make_async_copy(keys_from, keys_hbm.at[:, k], sems.at[0]).start()
        pltpu.make_async_copy(values_from, values_hbm.at[v], sems.at[1]).start()

    for i in range(1, 4):
        at = pl.ds(pl.multiple_of((last ^ i) * 2048, 2048), 2048)
        leave(keys.at[:, at], at, values.at[at], at)
    for i in range(4):
        for other in range(1, 4):
            at = pl.ds(place_of(last * 4 + i, lax.rem(pair + other, 4)), LANES)
            leave(keys.at[:, at], at, values.at[at], at)
    expand(
        rows, pair, range(12, 16), [LANES * i for i in range(4)], gain, w, xn, last_keys, last_values
    )
    for i in range(4):
        here, at = pl.ds(LANES * i, LANES), pl.ds(places[i], LANES)
        leave(last_keys.at[:, here], at, last_values.at[here], at)
    pltpu.make_async_copy(keys, keys_hbm, sems.at[0]).wait()
    pltpu.make_async_copy(values, values_hbm, sems.at[1]).wait()


def shards(latents, rotary_rows, latent_gain, key_up, value_up):
    hbm = pl.BlockSpec(memory_space=pltpu.HBM)
    vmem = pl.BlockSpec(memory_space=pltpu.VMEM)
    dma, bf16, f32 = pltpu.SemaphoreType.DMA, jnp.bfloat16, jnp.float32
    keys_shape = jax.ShapeDtypeStruct((192, 8192), bf16)
    values_shape = jax.ShapeDtypeStruct((8192, 128), bf16)
    ready = pl.pallas_call(
        exchange,
        out_shape=(
            jax.ShapeDtypeStruct((16, 16, TALL, LANES), bf16),
            keys_shape,
            values_shape,
            jax.ShapeDtypeStruct((DEPTH, 2 * LANES), bf16),
            jax.ShapeDtypeStruct((1, DEPTH), f32),
        ),
        in_specs=[hbm] * 5,
        out_specs=(vmem,) * 5,
        scratch_shapes=[
            pltpu.VMEM((16, TALL, LANES), bf16),
            pltpu.VMEM((16, WIDE, 64), bf16),
            pltpu.VMEM((512, DEPTH), bf16),
            pltpu.VMEM((len(FAR), TALL, LANES), bf16),
            pltpu.VMEM((len(FAR), TALL, LANES), bf16),
            dma((4,)), dma, dma, dma((2,)), dma,
            dma((11,)), dma((16,)), dma((16,)), dma((16,)), dma((2,)),
            pltpu.SemaphoreType.REGULAR((3,)),
        ],
        compiler_params=pltpu.CompilerParams(
            collective_id=0, has_side_effects=True, vmem_limit_bytes=8 * 1024 * 1024
        ),
        cost_estimate=pl.CostEstimate(flops=2 * 8192 * 512 * 256, bytes_accessed=1 << 20, transcendentals=0),
    )(
        *(
            pltpu.with_memory_space_constraint(a, pltpu.HBM)
            for a in (
                latents,
                rotary_rows,
                latent_gain.reshape(1, DEPTH),
                key_up.reshape(DEPTH, LANES),
                value_up.reshape(DEPTH, LANES),
            )
        )
    )
    keys, values = pl.pallas_call(
        finish,
        out_shape=(keys_shape, values_shape),
        in_specs=[vmem] * 5,
        out_specs=(hbm, hbm),
        scratch_shapes=[
            pltpu.VMEM((512, DEPTH), bf16),
            pltpu.VMEM((192, 512), bf16),
            pltpu.VMEM((512, LANES), bf16),
            dma((2,)),
        ],
        compiler_params=pltpu.CompilerParams(vmem_limit_bytes=4 * 1024 * 1024),
    )(*ready)
    return keys.reshape(1, 1, 192, 8192), values.reshape(1, 8192, 1, 128)


def solution(mesh):
    placed = (
        P(None, ("span", "model"), None),
        P(None, ("span", "model"), None),
        P(),
        P(None, "model", None),
        P(None, "model", None),
    )
    return jax.shard_map(
        shards,
        mesh=mesh,
        in_specs=placed,
        out_specs=(P("span", "model", None, None), P("span", None, "model", None)),
        check_vma=False,
    )
```

```python
import functools

import jax
import jax.numpy as jnp
from jax import lax
from jax.experimental import pallas as pl
from jax.experimental.pallas import tpu as pltpu
from jax.sharding import PartitionSpec as P

MESH = pl.DeviceIdType.MESH
LANES = 128
WIDE = 32
GROUPS = 4
DEPTH = GROUPS * LANES
TALL = GROUPS * WIDE + WIDE // 2
MASKS = (0, 1, 3, 4, 12, 5, 7, 13, 2, 15, 6, 14, 8, 9, 10, 11)
NEAR, MIDDLE, FAR = (1, 2, 3, 4), (5, 6, 7, 8, 9, 12), (10, 11, 13, 14, 15)
RISING = (2, 2, 1, 1)


def normalized(rows, pair, slot, gain, xn, at):
    blocks = [rows[4 * pair + b, slot] for b in range(4)]
    x = [
        jnp.concatenate([b[g * WIDE : (g + 1) * WIDE] for b in blocks], axis=0).astype(jnp.float32)
        for g in range(GROUPS)
    ]
    squares = functools.reduce(lambda a, b: a + b, [v * v for v in x])
    scale = lax.rsqrt(jnp.sum(squares, axis=-1, keepdims=True) / DEPTH + 1e-06)
    for g in range(GROUPS):
        lanes = slice(g * LANES, (g + 1) * LANES)
        xn[at : at + LANES, lanes] = (x[g] * scale * gain[:, lanes]).astype(jnp.bfloat16)
    turned = []
    for b in blocks:
        packed = b[GROUPS * WIDE :].astype(jnp.float32)
        turned += [packed, pltpu.roll(packed, LANES // 2, 1)]
    return jnp.concatenate(turned, axis=0).astype(jnp.bfloat16)


def expand(rows, pair, slots, places, gain, w, xn, keys, values):
    rotary = [normalized(rows, pair, s, gain, xn, LANES * i) for i, s in enumerate(slots)]
    both = jnp.dot(xn[...], w[...], preferred_element_type=jnp.float32).astype(jnp.bfloat16)
    for i, at in enumerate(places):
        part = both[LANES * i : LANES * (i + 1)]
        values[pl.ds(at, LANES), :] = part[:, LANES:]
        keys[:LANES, pl.ds(at, LANES)] = part[:, :LANES].T
        keys[LANES:, pl.ds(at, LANES)] = rotary[i].T[: LANES // 2]


def falling(part):
    start, size = 4 * part + RISING[part], 4 - RISING[part]
    if part < 3:
        return [(start, size, 12 + part)]
    return [(start, size - 1, 15), (start + size - 1, 1, 16)]


def place_of(source, pair):
    return pl.multiple_of(source * 512 + pair * LANES, LANES)


def mask_of(group, i):
    a, b, c, d = (MASKS[4 * g + i] for g in range(4))
    return jnp.where(group == 0, a, jnp.where(group == 1, b, jnp.where(group == 2, c, d)))


def exchange(
    lat_hbm, rot_hbm, gain_hbm, wk_hbm, wv_hbm,
    rows, keys, values, w, gain,
    pack, rot, xn, stage_up, stage_down,
    in_sems, a_send, r_send, z_send, c_send, a_recv, p_recv, m_recv, c_recv, stage_recv, token,
):
    span, model = lax.axis_index("span"), lax.axis_index("model")
    z, c = model // 2, lax.rem(model, 2)
    up = lax.rem(model + 2, 16)
    down = lax.rem(model + 14, 16)
    other = model + 1 - 2 * c

    barrier = pltpu.get_barrier_semaphore()
    for m in (up, down, other):
        pl.semaphore_signal(barrier, inc=1, device_id=(span, m), device_id_type=MESH)
    near = [span ^ MASKS[slot] for slot in NEAR]
    for s in near:
        pl.semaphore_signal(barrier, inc=1, device_id=(s, model), device_id_type=MESH)

    pltpu.make_async_copy(rot_hbm, rot, in_sems.at[0]).start()
    for g in range(GROUPS):
        pltpu.make_async_copy(
            lat_hbm.at[:, :, pl.ds(g * LANES, LANES)],
            pack.at[:, pl.ds(g * WIDE, WIDE), :],
            in_sems.at[1],
        ).start()
    pltpu.make_async_copy(gain_hbm, gain, in_sems.at[2]).start()
    pltpu.make_async_copy(wk_hbm, w.at[:, pl.ds(0, LANES)], in_sems.at[3]).start()
    pltpu.make_async_copy(wv_hbm, w.at[:, pl.ds(LANES, LANES)], in_sems.at[3]).start()
    pltpu.make_async_copy(rot_hbm, rot, in_sems.at[0]).wait()
    half = WIDE // 2
    pack[:, GROUPS * WIDE :, :] = jnp.concatenate([rot[:, :half, :], rot[:, half:, :]], axis=-1)
    landed = pack.at[:, pl.ds(0, GROUPS * WIDE), :]
    pltpu.make_async_copy(landed, landed, in_sems.at[1]).wait()
    pl.semaphore_wait(barrier, 7)

    def send(src, dst, send_sem, recv_sem, s, m):
        return pltpu.make_async_remote_copy(
            src_ref=src, dst_ref=dst, send_sem=send_sem, recv_sem=recv_sem,
            device_id=(s, m), device_id_type=MESH,
        )

    def arrived(count, sem):
        piece = rows.at[0, pl.ds(0, count)]
        send(piece, piece, c_send, sem, span, other).wait_recv()

    def upward(src, dst, zs, sem):
        send(src, dst, z_send.at[zs], sem, span, up).start()

    def downward(src, dst, zs, sem):
        send(src, dst, z_send.at[zs], sem, span, down).start()

    def across(src, dst, sem):
        send(src, dst, c_send, sem, span, other).start()

    def spread(slot, sem):
        to = span ^ MASKS[slot]
        send(pack.at[to], rows.at[model, slot], a_send, a_recv.at[sem], to, model).start()

    def onward(slot, sem):
        arrived(1, a_recv.at[sem])
        piece = rows.at[model, slot]
        upward(piece, piece, 0, p_recv.at[slot // 4])
        downward(piece, piece, 0, m_recv.at[slot // 4])

    def tell(turn):
        for s in near:
            pl.semaphore_signal(token.at[turn], inc=1, device_id=(s, model), device_id_type=MESH)

    first, first_at = pack.at[span], rows.at[model, 0]
    upward(first, first_at, 0, p_recv.at[0])
    downward(first, first_at, 0, m_recv.at[0])
    for i, slot in enumerate(NEAR):
        spread(slot, i)
    tell(0)
    for i, slot in enumerate(FAR):
        src = pack.at[span ^ MASKS[slot]]
        upward(src, stage_up.at[i], 0, stage_recv.at[0])
        downward(src, stage_down.at[i], 0, stage_recv.at[1])
    across(first, first_at, c_recv.at[0])
    rows[model, 0] = pack[span]
    pl.semaphore_wait(token.at[0], 4)
    for i, slot in enumerate(MIDDLE):
        spread(slot, 4 + i)
    tell(1)
    for i, slot in enumerate(NEAR):
        onward(slot, i)
    pl.semaphore_wait(token.at[1], 4)
    tell(2)
    for i, slot in enumerate(MIDDLE[:2]):
        onward(slot, 4 + i)
    pl.semaphore_wait(token.at[2], 4)
    for i, slot in enumerate(MIDDLE[2:]):
        onward(slot, 6 + i)

    for stage, sem, origin, recv in ((stage_up, 0, down, p_recv), (stage_down, 1, up, m_recv)):
        send(stage, stage, r_send, stage_recv.at[sem], span, up).wait_recv()
        for i, slot in enumerate(FAR):
            send(
                stage.at[i], rows.at[origin, slot], r_send, recv.at[slot // 4],
                span ^ MASKS[slot], model,
            ).start()
    for slot in FAR:
        spread(slot, 10)
    for start, count in ((1, 3), (4, 4), (8, 2), (12, 1)):
        piece = rows.at[model, pl.ds(start, count)]
        across(piece, piece, c_recv.at[start // 4])
    pltpu.make_async_copy(gain_hbm, gain, in_sems.at[2]).wait()
    pltpu.make_async_copy(w, w, in_sems.at[3]).wait()

    side = 1 - 2 * lax.rem(z, 2)

    def tile(t, j):
        shift = jnp.where(t == 0, 0, jnp.where(t == 1, 4 - side, jnp.where(t == 2, 4 + side, 2)))
        pair = lax.rem(z // 2 + shift, 4)
        expand(
            rows, pair, [4 * j + s for s in range(4)],
            [place_of(span ^ mask_of(j, s), pair) for s in range(4)],
            gain, w, xn, keys, values,
        )

    @pl.loop(0, 12)
    def _(n):
        t, j = n // 4, lax.rem(n, 4)
        mp = lax.rem(model + 30 - 2 * t, 16)
        mm = lax.rem(model + 2 + 2 * t, 16)
        from_below, from_above = rows.at[mp, pl.ds(4 * j, 4)], rows.at[mm, pl.ds(4 * j, 4)]
        arrived(4, p_recv.at[n])

        @pl.when(t < 2)
        def _():
            upward(from_below, from_below, 0, p_recv.at[n + 4])

        for part, count in enumerate(RISING):

            @pl.when(n == 8 + part)
            def _():
                piece = rows.at[mp, pl.ds(4 * part, count)]
                upward(piece, piece, 1, p_recv.at[12 + part])

        arrived(4, m_recv.at[n])

        @pl.when(t < 2)
        def _():
            downward(from_above, from_above, 0, m_recv.at[n + 4])

        for part, count in enumerate(RISING):

            @pl.when(n == 8 + part)
            def _():
                for start, size, sem in falling(part):
                    piece = rows.at[mm, pl.ds(start, size)]
                    downward(piece, piece, 1, m_recv.at[sem])

        @pl.when(n == 2)
        def _():
            arrived(5, a_recv.at[10])
            for start, count in ((10, 2), (13, 3)):
                piece = rows.at[model, pl.ds(start, count)]
                across(piece, piece, c_recv.at[start // 4])

        across(from_below, from_below, c_recv.at[n])
        across(from_above, from_above, c_recv.at[n])

        @pl.when(n >= 1)
        def _():
            i = n - 1

            @pl.when(i < 4)
            def _():
                arrived(12, c_recv.at[i])

            @pl.when(i >= 4)
            def _():
                arrived(8, c_recv.at[i])

            tile(i // 4, lax.rem(i, 4))

    opposite = lax.rem(model + 8, 16)
    for part, count in enumerate(RISING):
        low = rows.at[opposite, pl.ds(4 * part, count)]
        arrived(count, p_recv.at[12 + part])
        across(low, low, c_recv.at[12 + part])
        for start, size, sem in falling(part):
            high = rows.at[opposite, pl.ds(start, size)]
            arrived(size, m_recv.at[sem])
            across(high, high, c_recv.at[12 + part])
        if part == 0:
            arrived(8, c_recv.at[11])
            tile(2, 3)
        else:
            arrived(4, c_recv.at[11 + part])
            tile(3, part - 1)
    arrived(4, c_recv.at[15])

    send(pack.at[pl.ds(0, 15)], rows.at[0, pl.ds(0, 15)], a_send, a_recv.at[0], span, other).wait_send()
    send(rows.at[0, pl.ds(0, 10)], rows.at[0, pl.ds(0, 10)], r_send, a_recv.at[0], span, other).wait_send()
    send(rows.at[pl.ds(0, 6)], rows.at[pl.ds(0, 6)], z_send.at[0], a_recv.at[0], span, other).wait_send()
    send(rows.at[0], rows.at[0], z_send.at[1], a_recv.at[0], span, other).wait_send()
    send(rows.at[pl.ds(0, 8)], rows.at[pl.ds(0, 8)], c_send, a_recv.at[0], span, other).wait_send()


def finish(
    rows, keys_in, values_in, w, gain, keys_hbm, values_hbm, keys, values, xn, sems
):
    span, model = lax.axis_index("span"), lax.axis_index("model")
    last = (span // 4) ^ 2
    pair = lax.rem(model // 4 + 2, 4)

    def leave(part):
        at = pl.ds(pl.multiple_of(part * 2048, 2048), 2048)
        pltpu.make_async_copy(keys.at[:, at], keys_hbm.at[:, at], sems.at[0]).start()
        pltpu.make_async_copy(values.at[at], values_hbm.at[at], sems.at[1]).start()

    for i in range(1, 4):
        leave(last ^ i)
    expand(
        rows, pair, range(12, 16), [place_of(span ^ mask, pair) for mask in MASKS[12:]],
        gain, w, xn, keys, values,
    )
    leave(last)
    pltpu.make_async_copy(keys, keys_hbm, sems.at[0]).wait()
    pltpu.make_async_copy(values, values_hbm, sems.at[1]).wait()


def shards(latents, rotary_rows, latent_gain, key_up, value_up):
    hbm = pl.BlockSpec(memory_space=pltpu.HBM)
    vmem = pl.BlockSpec(memory_space=pltpu.VMEM)
    dma, bf16, f32 = pltpu.SemaphoreType.DMA, jnp.bfloat16, jnp.float32
    keys_shape = jax.ShapeDtypeStruct((192, 8192), bf16)
    values_shape = jax.ShapeDtypeStruct((8192, 128), bf16)
    ready = pl.pallas_call(
        exchange,
        out_shape=(
            jax.ShapeDtypeStruct((16, 16, TALL, LANES), bf16),
            keys_shape,
            values_shape,
            jax.ShapeDtypeStruct((DEPTH, 2 * LANES), bf16),
            jax.ShapeDtypeStruct((1, DEPTH), f32),
        ),
        in_specs=[hbm] * 5,
        out_specs=(vmem,) * 5,
        scratch_shapes=[
            pltpu.VMEM((16, TALL, LANES), bf16),
            pltpu.VMEM((16, WIDE, 64), bf16),
            pltpu.VMEM((512, DEPTH), bf16),
            pltpu.VMEM((len(FAR), TALL, LANES), bf16),
            pltpu.VMEM((len(FAR), TALL, LANES), bf16),
            dma((4,)), dma, dma, dma((2,)), dma,
            dma((11,)), dma((16,)), dma((17,)), dma((16,)), dma((2,)),
            pltpu.SemaphoreType.REGULAR((3,)),
        ],
        compiler_params=pltpu.CompilerParams(
            collective_id=0, has_side_effects=True, vmem_limit_bytes=8 * 1024 * 1024
        ),
        cost_estimate=pl.CostEstimate(flops=2 * 8192 * 512 * 256, bytes_accessed=1 << 20, transcendentals=0),
    )(
        *(
            pltpu.with_memory_space_constraint(a, pltpu.HBM)
            for a in (
                latents,
                rotary_rows,
                latent_gain.reshape(1, DEPTH),
                key_up.reshape(DEPTH, LANES),
                value_up.reshape(DEPTH, LANES),
            )
        )
    )
    keys, values, _, _ = pl.pallas_call(
        finish,
        out_shape=(keys_shape, values_shape) * 2,
        in_specs=[vmem] * 5,
        out_specs=(hbm, hbm, vmem, vmem),
        scratch_shapes=[pltpu.VMEM((512, DEPTH), bf16), dma((2,))],
        input_output_aliases={1: 2, 2: 3},
        compiler_params=pltpu.CompilerParams(vmem_limit_bytes=4 * 1024 * 1024),
    )(*ready)
    return keys.reshape(1, 1, 192, 8192), values.reshape(1, 8192, 1, 128)


def solution(mesh):
    placed = (
        P(None, ("span", "model"), None),
        P(None, ("span", "model"), None),
        P(),
        P(None, "model", None),
        P(None, "model", None),
    )
    return jax.shard_map(
        shards,
        mesh=mesh,
        in_specs=placed,
        out_specs=(P("span", "model", None, None), P("span", None, "model", None)),
        check_vma=False,
    )
```

```python
import functools

import jax
import jax.numpy as jnp
from jax import lax
from jax.experimental import pallas as pl
from jax.experimental.pallas import tpu as pltpu
from jax.sharding import PartitionSpec as P

MESH = pl.DeviceIdType.MESH
LANES = 128
WIDE = 32
GROUPS = 4
DEPTH = GROUPS * LANES
TALL = GROUPS * WIDE + WIDE // 2
MASKS = (0, 1, 3, 4, 12, 5, 7, 13, 2, 15, 6, 14, 8, 9, 10, 11)
NEAR, MIDDLE, FAR = (1, 2, 3, 4), (5, 6, 7, 8, 9, 12), (10, 11, 13, 14, 15)
RISING = (2, 2, 1, 1)


def normalized(rows, pair, slot, gain, xn, at):
    blocks = [rows[4 * pair + b, slot] for b in range(4)]
    x = [
        jnp.concatenate([b[g * WIDE : (g + 1) * WIDE] for b in blocks], axis=0).astype(jnp.float32)
        for g in range(GROUPS)
    ]
    squares = functools.reduce(lambda a, b: a + b, [v * v for v in x])
    scale = lax.rsqrt(jnp.sum(squares, axis=-1, keepdims=True) / DEPTH + 1e-06)
    for g in range(GROUPS):
        lanes = slice(g * LANES, (g + 1) * LANES)
        xn[at : at + LANES, lanes] = (x[g] * scale * gain[:, lanes]).astype(jnp.bfloat16)
    turned = []
    for b in blocks:
        packed = b[GROUPS * WIDE :].astype(jnp.float32)
        turned += [packed, pltpu.roll(packed, LANES // 2, 1)]
    return jnp.concatenate(turned, axis=0).astype(jnp.bfloat16)


def expand(rows, pair, slots, places, gain, w, xn, keys, values):
    rotary = [normalized(rows, pair, s, gain, xn, LANES * i) for i, s in enumerate(slots)]
    both = jnp.dot(xn[...], w[...], preferred_element_type=jnp.float32).astype(jnp.bfloat16)
    for i, at in enumerate(places):
        part = both[LANES * i : LANES * (i + 1)]
        values[pl.ds(at, LANES), :] = part[:, LANES:]
        keys[:LANES, pl.ds(at, LANES)] = part[:, :LANES].T
        keys[LANES:, pl.ds(at, LANES)] = rotary[i].T[: LANES // 2]


def falling(part):
    start, size = 4 * part + RISING[part], 4 - RISING[part]
    if part < 3:
        return [(start, size, 8 + part)]
    return [(start, size - 1, 11), (start + size - 1, 1, 12)]


def place_of(source, pair):
    return pl.multiple_of(source * 512 + pair * LANES, LANES)


def mask_of(group, i):
    a, b, c, d = (MASKS[4 * g + i] for g in range(4))
    return jnp.where(group == 0, a, jnp.where(group == 1, b, jnp.where(group == 2, c, d)))


def exchange(
    lat_hbm, rot_hbm, gain_hbm, wk_hbm, wv_hbm,
    rows, keys, values, w, gain,
    pack, rot, xn, stage_up, stage_down,
    in_sems, a_send, r_send, z_send, c_send, a_recv, p_recv, m_recv, c_recv, stage_recv, token,
):
    span, model = lax.axis_index("span"), lax.axis_index("model")
    z, c = model // 2, lax.rem(model, 2)
    up = lax.rem(model + 2, 16)
    down = lax.rem(model + 14, 16)
    other = model + 1 - 2 * c

    barrier = pltpu.get_barrier_semaphore()
    for m in (up, down, other):
        pl.semaphore_signal(barrier, inc=1, device_id=(span, m), device_id_type=MESH)
    near = [span ^ MASKS[slot] for slot in NEAR]
    for s in near:
        pl.semaphore_signal(barrier, inc=1, device_id=(s, model), device_id_type=MESH)

    pltpu.make_async_copy(rot_hbm, rot, in_sems.at[0]).start()
    for g in range(GROUPS):
        pltpu.make_async_copy(
            lat_hbm.at[:, :, pl.ds(g * LANES, LANES)],
            pack.at[:, pl.ds(g * WIDE, WIDE), :],
            in_sems.at[1],
        ).start()
    pltpu.make_async_copy(gain_hbm, gain, in_sems.at[2]).start()
    pltpu.make_async_copy(wk_hbm, w.at[:, pl.ds(0, LANES)], in_sems.at[3]).start()
    pltpu.make_async_copy(wv_hbm, w.at[:, pl.ds(LANES, LANES)], in_sems.at[3]).start()
    pltpu.make_async_copy(rot_hbm, rot, in_sems.at[0]).wait()
    half = WIDE // 2
    pack[:, GROUPS * WIDE :, :] = jnp.concatenate([rot[:, :half, :], rot[:, half:, :]], axis=-1)
    landed = pack.at[:, pl.ds(0, GROUPS * WIDE), :]
    pltpu.make_async_copy(landed, landed, in_sems.at[1]).wait()
    pl.semaphore_wait(barrier, 7)

    def send(src, dst, send_sem, recv_sem, s, m):
        return pltpu.make_async_remote_copy(
            src_ref=src, dst_ref=dst, send_sem=send_sem, recv_sem=recv_sem,
            device_id=(s, m), device_id_type=MESH,
        )

    def arrived(count, sem):
        piece = rows.at[0, pl.ds(0, count)]
        send(piece, piece, c_send, sem, span, other).wait_recv()

    def upward(src, dst, zs, sem):
        send(src, dst, z_send.at[zs], sem, span, up).start()

    def downward(src, dst, zs, sem):
        send(src, dst, z_send.at[zs], sem, span, down).start()

    def across(src, dst, sem):
        send(src, dst, c_send, sem, span, other).start()

    def spread(slot, sem):
        to = span ^ MASKS[slot]
        send(pack.at[to], rows.at[model, slot], a_send, a_recv.at[sem], to, model).start()

    def onward(slot, sem):
        arrived(1, a_recv.at[sem])
        piece = rows.at[model, slot]
        upward(piece, piece, 0, p_recv.at[slot // 4])
        downward(piece, piece, 0, m_recv.at[slot // 4])

    def tell(turn):
        for s in near:
            pl.semaphore_signal(token.at[turn], inc=1, device_id=(s, model), device_id_type=MESH)

    first, first_at = pack.at[span], rows.at[model, 0]
    upward(first, first_at, 0, p_recv.at[0])
    downward(first, first_at, 0, m_recv.at[0])
    for i, slot in enumerate(NEAR):
        spread(slot, i)
    tell(0)
    for i, slot in enumerate(FAR):
        src = pack.at[span ^ MASKS[slot]]
        upward(src, stage_up.at[i], 0, stage_recv.at[0])
        downward(src, stage_down.at[i], 0, stage_recv.at[1])
    across(first, first_at, c_recv.at[0])
    rows[model, 0] = pack[span]
    pl.semaphore_wait(token.at[0], 4)
    for i, slot in enumerate(MIDDLE):
        spread(slot, 4 + i)
    tell(1)
    for i, slot in enumerate(NEAR):
        onward(slot, i)
    pl.semaphore_wait(token.at[1], 4)
    tell(2)
    for i, slot in enumerate(MIDDLE[:2]):
        onward(slot, 4 + i)
    pl.semaphore_wait(token.at[2], 4)
    for i, slot in enumerate(MIDDLE[2:]):
        onward(slot, 6 + i)

    for stage, sem, origin, recv in ((stage_up, 0, down, p_recv), (stage_down, 1, up, m_recv)):
        send(stage, stage, r_send, stage_recv.at[sem], span, up).wait_recv()
        for i, slot in enumerate(FAR):
            send(
                stage.at[i], rows.at[origin, slot], r_send, recv.at[slot // 4],
                span ^ MASKS[slot], model,
            ).start()
    for slot in FAR:
        spread(slot, 10)
    for start, count in ((1, 3), (4, 4), (8, 2), (12, 1)):
        piece = rows.at[model, pl.ds(start, count)]
        across(piece, piece, c_recv.at[start // 4])
    pltpu.make_async_copy(gain_hbm, gain, in_sems.at[2]).wait()
    pltpu.make_async_copy(w, w, in_sems.at[3]).wait()

    side = 1 - 2 * lax.rem(z, 2)

    def tile(t, j):
        shift = jnp.where(t == 0, 0, jnp.where(t == 1, 4 - side, jnp.where(t == 2, 4 + side, 2)))
        pair = lax.rem(z // 2 + shift, 4)
        expand(
            rows, pair, [4 * j + s for s in range(4)],
            [place_of(span ^ mask_of(j, s), pair) for s in range(4)],
            gain, w, xn, keys, values,
        )

    @pl.loop(0, 4)
    def _(j):
        below, above = rows.at[down, pl.ds(4 * j, 4)], rows.at[up, pl.ds(4 * j, 4)]
        arrived(4, p_recv.at[j])
        upward(below, below, 0, p_recv.at[4 + j // 2])
        arrived(4, m_recv.at[j])
        downward(above, above, 0, m_recv.at[4 + j // 2])

        @pl.when(j == 2)
        def _():
            arrived(5, a_recv.at[10])
            for start, count in ((10, 2), (13, 3)):
                piece = rows.at[model, pl.ds(start, count)]
                across(piece, piece, c_recv.at[start // 4])

        across(below, below, c_recv.at[j])
        across(above, above, c_recv.at[j])

        @pl.when(j >= 1)
        def _():
            arrived(12, c_recv.at[j - 1])
            tile(0, j - 1)

    @pl.loop(0, 4)
    def _(q):
        t, half = 1 + q // 2, lax.rem(q, 2)
        mp = lax.rem(model + 30 - 2 * t, 16)
        mm = lax.rem(model + 2 + 2 * t, 16)
        below, above = rows.at[mp, pl.ds(8 * half, 8)], rows.at[mm, pl.ds(8 * half, 8)]
        arrived(8, p_recv.at[4 + q])

        @pl.when(t == 1)
        def _():
            upward(below, below, 0, p_recv.at[6 + half])

        for part, count in enumerate(RISING):

            @pl.when(q == 2 + part // 2)
            def _():
                piece = rows.at[mp, pl.ds(4 * part, count)]
                upward(piece, piece, 1, p_recv.at[8 + part])

        arrived(8, m_recv.at[4 + q])

        @pl.when(t == 1)
        def _():
            downward(above, above, 0, m_recv.at[6 + half])

        for part in range(4):

            @pl.when(q == 2 + part // 2)
            def _():
                for start, size, sem in falling(part):
                    piece = rows.at[mm, pl.ds(start, size)]
                    downward(piece, piece, 1, m_recv.at[sem])

        across(below, below, c_recv.at[4 + q])
        across(above, above, c_recv.at[4 + q])

        @pl.when(q == 0)
        def _():
            arrived(12, c_recv.at[3])
            tile(0, 3)

        @pl.when(q > 0)
        def _():
            arrived(16, c_recv.at[3 + q])

            @pl.loop(0, 2)
            def _(i):
                tile((q + 1) // 2, 2 * lax.rem(q - 1, 2) + i)

    opposite = lax.rem(model + 8, 16)
    for part, count in enumerate(RISING):
        low = rows.at[opposite, pl.ds(4 * part, count)]
        arrived(count, p_recv.at[8 + part])
        across(low, low, c_recv.at[8 + part])
        for start, size, sem in falling(part):
            high = rows.at[opposite, pl.ds(start, size)]
            arrived(size, m_recv.at[sem])
            across(high, high, c_recv.at[8 + part])
        if part == 0:
            arrived(16, c_recv.at[7])
            tile(2, 2)
            tile(2, 3)
        else:
            arrived(4, c_recv.at[7 + part])
            tile(3, part - 1)
    arrived(4, c_recv.at[11])

    send(pack.at[pl.ds(0, 15)], rows.at[0, pl.ds(0, 15)], a_send, a_recv.at[0], span, other).wait_send()
    send(rows.at[0, pl.ds(0, 10)], rows.at[0, pl.ds(0, 10)], r_send, a_recv.at[0], span, other).wait_send()
    send(rows.at[pl.ds(0, 6)], rows.at[pl.ds(0, 6)], z_send.at[0], a_recv.at[0], span, other).wait_send()
    send(rows.at[0], rows.at[0], z_send.at[1], a_recv.at[0], span, other).wait_send()
    send(rows.at[pl.ds(0, 8)], rows.at[pl.ds(0, 8)], c_send, a_recv.at[0], span, other).wait_send()


def finish(
    rows, keys_in, values_in, w, gain, keys_hbm, values_hbm, keys, values, xn, sems
):
    span, model = lax.axis_index("span"), lax.axis_index("model")
    last = (span // 4) ^ 2
    pair = lax.rem(model // 4 + 2, 4)

    def leave(part):
        at = pl.ds(pl.multiple_of(part * 2048, 2048), 2048)
        pltpu.make_async_copy(keys.at[:, at], keys_hbm.at[:, at], sems.at[0]).start()
        pltpu.make_async_copy(values.at[at], values_hbm.at[at], sems.at[1]).start()

    for i in range(1, 4):
        leave(last ^ i)
    expand(
        rows, pair, range(12, 16), [place_of(span ^ mask, pair) for mask in MASKS[12:]],
        gain, w, xn, keys, values,
    )
    leave(last)
    pltpu.make_async_copy(keys, keys_hbm, sems.at[0]).wait()
    pltpu.make_async_copy(values, values_hbm, sems.at[1]).wait()


def shards(latents, rotary_rows, latent_gain, key_up, value_up):
    hbm = pl.BlockSpec(memory_space=pltpu.HBM)
    vmem = pl.BlockSpec(memory_space=pltpu.VMEM)
    dma, bf16, f32 = pltpu.SemaphoreType.DMA, jnp.bfloat16, jnp.float32
    keys_shape = jax.ShapeDtypeStruct((192, 8192), bf16)
    values_shape = jax.ShapeDtypeStruct((8192, 128), bf16)
    ready = pl.pallas_call(
        exchange,
        out_shape=(
            jax.ShapeDtypeStruct((16, 16, TALL, LANES), bf16),
            keys_shape,
            values_shape,
            jax.ShapeDtypeStruct((DEPTH, 2 * LANES), bf16),
            jax.ShapeDtypeStruct((1, DEPTH), f32),
        ),
        in_specs=[hbm] * 5,
        out_specs=(vmem,) * 5,
        scratch_shapes=[
            pltpu.VMEM((16, TALL, LANES), bf16),
            pltpu.VMEM((16, WIDE, 64), bf16),
            pltpu.VMEM((512, DEPTH), bf16),
            pltpu.VMEM((len(FAR), TALL, LANES), bf16),
            pltpu.VMEM((len(FAR), TALL, LANES), bf16),
            dma((4,)), dma, dma, dma((2,)), dma,
            dma((11,)), dma((12,)), dma((13,)), dma((12,)), dma((2,)),
            pltpu.SemaphoreType.REGULAR((3,)),
        ],
        compiler_params=pltpu.CompilerParams(
            collective_id=0, has_side_effects=True, vmem_limit_bytes=8 * 1024 * 1024
        ),
        cost_estimate=pl.CostEstimate(flops=2 * 8192 * 512 * 256, bytes_accessed=1 << 20, transcendentals=0),
    )(
        *(
            pltpu.with_memory_space_constraint(a, pltpu.HBM)
            for a in (
                latents,
                rotary_rows,
                latent_gain.reshape(1, DEPTH),
                key_up.reshape(DEPTH, LANES),
                value_up.reshape(DEPTH, LANES),
            )
        )
    )
    keys, values, _, _ = pl.pallas_call(
        finish,
        out_shape=(keys_shape, values_shape) * 2,
        in_specs=[vmem] * 5,
        out_specs=(hbm, hbm, vmem, vmem),
        scratch_shapes=[pltpu.VMEM((512, DEPTH), bf16), dma((2,))],
        input_output_aliases={1: 2, 2: 3},
        compiler_params=pltpu.CompilerParams(vmem_limit_bytes=4 * 1024 * 1024),
    )(*ready)
    return keys.reshape(1, 1, 192, 8192), values.reshape(1, 8192, 1, 128)


def solution(mesh):
    placed = (
        P(None, ("span", "model"), None),
        P(None, ("span", "model"), None),
        P(),
        P(None, "model", None),
        P(None, "model", None),
    )
    return jax.shard_map(
        shards,
        mesh=mesh,
        in_specs=placed,
        out_specs=(P("span", "model", None, None), P("span", None, "model", None)),
        check_vma=False,
    )
```
